32 devices in a mesh: ctx: 2 (over y), dp: 16 (over z, x, core).
Axes of the slice: x: 2, y: 2, z: 4, core: 2. Of those that a mesh axis runs over, the one named last changes fastest.
Arguments:
- queries: bfloat16 [16, 256, 1024], P('dp', 'ctx'), may hold values from -20 to 20
- keys: bfloat16 [16, 256, 1024], P('dp', 'ctx'), may hold values from -4 to 4
- values: bfloat16 [16, 256, 1024], P('dp', 'ctx'), may hold values from -6 to 6
- d_mixed: bfloat16 [16, 256, 1024], P('dp', 'ctx'), may hold values from -6 to 6
- series_ids: int32 [16, 256], P('dp', 'ctx'), may hold values from 0 to 3, never falling along the last dimension, each value on 1 to 192 neighbouring positions
- variate_ids: int32 [16, 256], P('dp', 'ctx'), may hold values from 0 to 3
- variate_bias: float32 [2, 16], replicated, may hold values from -4 to 4
- w_out: bfloat16 [1024, 1024], P('dp'), may hold values from -0.1875 to 0.1875
Outputs:
- mixed: bfloat16 [16, 256, 1024], P('dp', 'ctx')
- q_grad: bfloat16 [16, 256, 1024], P('dp', 'ctx')
- k_grad: bfloat16 [16, 256, 1024], P('dp', 'ctx')
- v_grad: bfloat16 [16, 256, 1024], P('dp', 'ctx')
- w_grad: float32 [1024, 1024], P('dp')
- bias_grad: float32 [2, 16], replicated
The draws below stay inside these ranges and needn't reach their ends.
Inputs may be any that keep to these rules, and one draw needn't show every extreme that they name: `series_ids`: within a packed row series numbers never fall; each series spans 1 to 192 consecutive tokens and some series spans exactly 192.
All inputs are finite; a program needn't handle non-finite values.
Results may differ from the reference program's by a relative error of at most 0.015.
Values may be sent and summed in bfloat16 or wider, within the bound.
No kernel may reach another device: no remote copies, remote signals or barrier semaphores. Data moves between devices by JAX's collectives and lax.ppermute only.
A program may use at most 128 MiB of HBM per device.

```python
import math
import jax
import jax.numpy as jnp
import numpy as np
from jax import lax

D = 1024
HEADS = 16
HEAD_DIM = 64
VARIATES = 4
BATCH = 16
ROW = 256
SERIES = 4
MOST = 192


def pair_draw(key):
    base = jax.random.fold_in(key, 911)
    key_query, key_key = jax.random.split(base)
    shape = (BATCH, ROW, D)
    keys_drawn = jnp.clip(jax.random.normal(key_key, shape, jnp.float32), -4.0, 4.0)
    queries_drawn = jnp.clip(jax.random.normal(key_query, shape, jnp.float32), -4.0, 4.0)
    return (queries_drawn, keys_drawn)


def draw_queries(key, part):
    return pair_draw(key)[0].astype(jnp.bfloat16)


def draw_keys(key, part):
    return pair_draw(key)[1].astype(jnp.bfloat16)


def with_ends(entries, rng, smallest, high):
    index_at = [jax.random.randint(jax.random.fold_in(rng, axis), (), 0, length) for axis, length in enumerate(entries.shape)]
    widest = entries.shape.index(max(entries.shape))
    next_to = index_at[:widest] + [(index_at[widest] + 1) % entries.shape[widest]] + index_at[widest + 1:]
    return entries.at[tuple(index_at)].set(smallest).at[tuple(next_to)].set(high)


def spiked(values, key, source, target, blocks, factor):
    owner, partner = [(jnp.arange(values.shape[dim]) // (values.shape[dim] // blocks)).reshape([-1 if axis == dim else 1 for axis in range(values.ndim)]) for dim in (source, target)]
    chosen = jax.random.permutation(key, blocks)[partner]
    strong = (owner == chosen) | (owner == (partner + blocks // 2) % blocks)
    return jnp.where(strong, factor * values, values)


def block_levels(rng, shape, shards, smallest, high):
    level, own = 1.0, jax.random.fold_in(rng, 6)
    for position, shards_of in shards:
        heights = jnp.exp(jax.random.uniform(jax.random.fold_in(own, position), (shards_of,), jnp.float32, smallest / len(shards), high / len(shards)))
        level = level * jnp.repeat(heights, shape[position] // shards_of).reshape([-1 if axis == position else 1 for axis in range(len(shape))])
    return level


def profile(count, total, reach, lean):
    weights = [(1 << 20) // math.isqrt(standing ** lean) + 1 for standing in range(2, count + 1)]
    spare, counts = total - reach - (count - 1), [1] * (count - 1)
    while spare > 0:
        free = [i for i in range(count - 1) if counts[i] < reach]
        mass, left = sum([weights[i] for i in free]), spare
        for i in free:
            addition = min(reach - counts[i], max(1, left * weights[i] // mass), spare)
            counts[i] = counts[i] + addition
            spare = spare - addition
    return np.array([reach] + counts)


def uneven(rng, count, total, limit, skew):
    if count == 2:
        one = jax.random.randint(rng, (), max(1, total - limit), min(limit, total - 1) + 1)
        return jnp.stack([one, total - one])
    lengths = jnp.asarray(profile(count, total, limit, skew), jnp.int32)
    twos = (count - 1) // 2
    source_of, sink = lengths[1:1 + 2 * twos:2], lengths[2:2 + 2 * twos:2]
    room = jnp.minimum(source_of - 1, limit - sink)
    moved = jax.random.randint(jax.random.fold_in(rng, 1), (twos,), 0, 1 << 20) % (room + 1)
    lengths = lengths.at[1:1 + 2 * twos:2].set(source_of - moved).at[2:2 + 2 * twos:2].set(sink + moved)
    return lengths[jax.random.permutation(jax.random.fold_in(rng, 2), count)]


def bell_draw(key, shape, deviation, reach, shards=(), dtype=jnp.bfloat16):
    values = deviation * jax.random.normal(key, shape, jnp.float32)
    if shards:
        values = values * block_levels(key, shape, shards, -0.22, 0.18)
    return jnp.clip(values, -reach, reach).astype(dtype)


def gaussian_with(key, dims, deviation, bound, pieces, heavy, held_as=jnp.bfloat16):
    values = deviation * jax.random.normal(key, dims, jnp.float32)
    if pieces:
        values = values * block_levels(key, dims, pieces, -0.22, 0.18)
    return jnp.clip(spiked(values, jax.random.fold_in(key, 3), *heavy), -bound, bound).astype(held_as)


def setup_inputs(seed: int = 0) -> dict:
    splits = jax.random.split(jax.random.key(seed), 9)
    queries = draw_queries(jax.random.fold_in(splits[8], 71), 0)
    keys = draw_keys(jax.random.fold_in(splits[8], 71), 0)
    values = gaussian_with(splits[2], (BATCH, ROW, D), 1.0, 6.0, ((0, 16), (1, 2)), (0, 2, 16, 2.0))
    d_mixed = bell_draw(splits[3], (BATCH, ROW, D), 1.0, 6.0, ((0, 16), (1, 2)))
    series_ids = jax.vmap(lambda own: jnp.searchsorted(jnp.cumsum(uneven(own, SERIES, ROW, MOST, 2)), jnp.arange(ROW), side="right"))(jax.random.split(splits[4], BATCH)).reshape((BATCH, ROW)).astype(jnp.int32)
    variate_ids = with_ends(jax.random.randint(splits[5], (BATCH, ROW), 0, VARIATES), jax.random.fold_in(splits[5], 1), 0, VARIATES - 1).astype(jnp.int32)
    variate_bias = bell_draw(splits[6], (2, HEADS), 1.0, 4.0, (), jnp.float32)
    w_out = bell_draw(splits[7], (D, D), D ** -0.5, 0.1875, ((0, 16),))
    return dict(queries=queries, keys=keys, values=values, d_mixed=d_mixed, series_ids=series_ids, variate_ids=variate_ids, variate_bias=variate_bias, w_out=w_out)


NEG = -1e30


def barrier_round(values):
    return lax.optimization_barrier(values.astype(jnp.bfloat16)).astype(jnp.float32)


def reference(queries, keys, values, d_mixed, series_ids, variate_ids, variate_bias, w_out):
    scale = HEAD_DIM ** -0.5

    def one_row(carry, row):
        w_sum, b_sum = carry
        query, key_rows, value_rows, upstream, series, variate = row
        qf = query.astype(jnp.float32).reshape(ROW, HEADS, HEAD_DIM)
        kf = key_rows.astype(jnp.float32).reshape(ROW, HEADS, HEAD_DIM)
        vf = value_rows.astype(jnp.float32).reshape(ROW, HEADS, HEAD_DIM)
        allowed = (series[:, None] == series[None, :])[None]
        same = (variate[:, None] == variate[None, :])[None]
        addend = jnp.where(same, variate_bias[0][:, None, None], variate_bias[1][:, None, None])
        scores = jnp.einsum("qhd,khd->hqk", qf, kf) * scale + addend
        scores = jnp.where(allowed, scores, NEG)
        top = jnp.max(scores, axis=2, keepdims=True)
        total = jnp.sum(jnp.where(allowed, jnp.exp(scores - top), 0.0), axis=2, keepdims=True)
        lse = top + jnp.log(total)
        probs = jnp.where(allowed, jnp.exp(scores - lse), 0.0)
        weights = barrier_round(probs)
        context = jnp.einsum("hqk,khd->qhd", weights, vf)
        context_bf = context.reshape(ROW, D).astype(jnp.bfloat16)
        mixed = jnp.dot(context_bf, w_out, preferred_element_type=jnp.float32).astype(jnp.bfloat16)
        d_context = jnp.dot(upstream, w_out.T, preferred_element_type=jnp.float32).astype(jnp.bfloat16)
        w_sum = w_sum + jnp.dot(context_bf.T, upstream, preferred_element_type=jnp.float32)
        df = d_context.astype(jnp.float32).reshape(ROW, HEADS, HEAD_DIM)
        delta = jnp.einsum("qhd,qhd->hq", df, context)
        dprob = jnp.einsum("qhd,khd->hqk", df, vf)
        dscore = probs * (dprob - delta[:, :, None])
        dround = barrier_round(dscore)
        q_grad = (jnp.einsum("hqk,khd->qhd", dround, kf) * scale).reshape(ROW, D).astype(jnp.bfloat16)
        k_grad = (jnp.einsum("hqk,qhd->khd", dround, qf) * scale).reshape(ROW, D).astype(jnp.bfloat16)
        v_grad = jnp.einsum("hqk,qhd->khd", weights, df).reshape(ROW, D).astype(jnp.bfloat16)
        b_row = jnp.stack([jnp.sum(jnp.where(same, dscore, 0.0), axis=(1, 2)),
                           jnp.sum(jnp.where(same, 0.0, dscore), axis=(1, 2))])
        return (w_sum, b_sum + b_row), (mixed, q_grad, k_grad, v_grad)

    start = (jnp.zeros((D, D), jnp.float32), jnp.zeros((2, HEADS), jnp.float32))
    (w_grad, bias_grad), (mixed, q_grad, k_grad, v_grad) = lax.scan(
        one_row, start, (queries, keys, values, d_mixed, series_ids, variate_ids))
    return mixed, q_grad, k_grad, v_grad, w_grad, bias_grad
```

```python
import functools

import jax
import jax.numpy as jnp
from jax import lax
from jax.experimental import pallas as pl
from jax.experimental.pallas import tpu as pltpu
from jax.sharding import PartitionSpec as P


HEADS = 16
HEAD_DIM = 64
GROUP = 4
PAIR = GROUP * HEAD_DIM
SCALE = HEAD_DIM ** -0.5
NEG = -1e30
BF = jnp.bfloat16
F32 = jnp.float32


def dot_nt(a, b):
    return lax.dot_general(a, b, (((1,), (1,)), ((), ())), preferred_element_type=F32)


def dot_tn(a, b):
    return lax.dot_general(a, b, (((0,), (0,)), ((), ())), preferred_element_type=F32)


def dot_nn(a, b):
    return lax.dot_general(a, b, (((1,), (0,)), ((), ())), preferred_element_type=F32)


def both(own_ref, oth_ref):
    return jnp.concatenate([own_ref[...], oth_ref[...]], axis=0)


def id_masks(own_ref, oth_ref):
    row = jnp.concatenate([own_ref[...], oth_ref[...]], axis=1)
    col = jnp.transpose(jnp.broadcast_to(row, (128, row.shape[1])))[:, :1]
    return row, col


def forward_kernel(bias_ref, ido_ref, idx_ref, qo_ref, qx_ref, ko_ref, kx_ref, vo_ref, vx_ref,
                   ctx_ref, wo_ref, wx_ref, neg_ref, same_ref):
    pair = pl.program_id(0)
    tok = qo_ref.shape[0]
    n = neg_ref.shape[0] // tok

    @pl.when(pair == 0)
    def _():
        row, col = id_masks(ido_ref, idx_ref)
        neg_ref[...] = jnp.where((row >> 8) == (col >> 8), 0.0, NEG)
        same_ref[...] = jnp.where((row & 255) == (col & 255), 1.0, 0.0)

    q = both(qo_ref, qx_ref)
    k = both(ko_ref, kx_ref)
    v = both(vo_ref, vx_ref)
    for half in range(GROUP):
        head = GROUP * pair + half
        gap = bias_ref[0, head] - bias_ref[1, head]
        lanes = slice(half * HEAD_DIM, (half + 1) * HEAD_DIM)
        qh = q[:, lanes] * jnp.asarray(SCALE, BF)
        kh, vh = k[:, lanes], v[:, lanes]
        for chunk in range(n):
            rows = slice(chunk * tok, (chunk + 1) * tok)
            s = dot_nt(qh[rows], kh) + (same_ref[rows, :] * gap + neg_ref[rows, :])
            e = jnp.exp(s - jnp.max(s, axis=1, keepdims=True))
            w = (e * (1.0 / jnp.sum(e, axis=1, keepdims=True))).astype(BF)
            ctx_ref[rows, lanes] = dot_nn(w, vh)
            if chunk == 0:
                wo_ref[half] = w
            else:
                wx_ref[half, (chunk - 1) * tok:chunk * tok, :] = w[:, :tok]


def weight_kernel(where_ref, ctx_ref, do_ref, dx_ref, keep_ref, send_ref):
    grads = dot_tn(ctx_ref[...].astype(BF), both(do_ref, dx_ref))
    nb, block, cols = keep_ref.shape
    grads = grads.reshape(nb, 2, block, cols)
    low = where_ref[1] == 0
    keep_ref[...] = jnp.where(low, grads[:, 0], grads[:, 1])
    send_ref[...] = jnp.where(low, grads[:, 1], grads[:, 0]).astype(BF)


def backward_kernel(pieces, where_ref, ido_ref, idx_ref, do_ref, dx_ref, qo_ref, qx_ref, ko_ref,
                    kx_ref, vo_ref, vx_ref, ctx_ref, wo_ref, wx_ref, *rest):
    piece_refs = rest[:len(pieces)]
    mixed_ref, qg_ref, kg_ref, vg_ref, bg_ref, wbuf_ref, same_ref, acc_ref, dall_ref = rest[len(pieces):]
    pair = pl.program_id(0)
    tok = qo_ref.shape[0]
    block = wbuf_ref.shape[2]
    nb = PAIR // (2 * block)

    @pl.when(pair == 0)
    def _():
        row, col = id_masks(ido_ref, idx_ref)
        same_ref[...] = jnp.where((row & 255) == (col[:tok] & 255), 1.0, 0.0)
        acc_ref[...] = jnp.zeros_like(acc_ref)
        dall_ref[...] = both(do_ref, dx_ref)
        for piece, ref in zip(pieces, piece_refs):
            index = jnp.bitwise_xor(where_ref[2], piece)
            wbuf_ref[index // 2, index % 2] = ref[...]

    w = wbuf_ref[pl.ds(pair * nb, nb)].reshape(PAIR, wbuf_ref.shape[3])
    d_pair = dot_nt(dall_ref[...], w).astype(BF)
    ctx = ctx_ref[...]
    acc_ref[...] += dot_nn(ctx[:tok].astype(BF), w)
    prod = d_pair.astype(F32) * ctx
    q = both(qo_ref, qx_ref) * jnp.asarray(SCALE, BF)
    k = both(ko_ref, kx_ref)
    v = both(vo_ref, vx_ref)
    same = same_ref[...]
    for half in range(GROUP):
        lanes = slice(half * HEAD_DIM, (half + 1) * HEAD_DIM)
        dh, qh, kh, vh = d_pair[:, lanes], q[:, lanes], k[:, lanes], v[:, lanes]
        delta = jnp.sum(prod[:, lanes], axis=1, keepdims=True)
        wo, wx = wo_ref[half], wx_ref[half]
        ds = wo.astype(F32) * (dot_nt(dh[:tok], vh) - delta[:tok])
        bg_ref[0, 2 * half:2 * half + 1, :] = jnp.sum(ds * same, axis=0, keepdims=True)
        bg_ref[0, 2 * half + 1:2 * half + 2, :] = jnp.sum(ds, axis=0, keepdims=True)
        ds = ds.astype(BF)
        qg_ref[:, lanes] = (dot_nn(ds, kh) * SCALE).astype(BF)
        dx = (wx.astype(F32) * (dot_nt(dh[tok:], vh[:tok]) - delta[tok:])).astype(BF)
        kg_ref[:, lanes] = (dot_tn(ds[:, :tok], qh[:tok]) + dot_tn(dx, qh[tok:])).astype(BF)
        vg_ref[:, lanes] = (dot_tn(wo[:, :tok], dh[:tok]) + dot_tn(wx, dh[tok:])).astype(BF)

    @pl.when(pair == pl.num_programs(0) - 1)
    def _():
        mixed_ref[...] = acc_ref[...].astype(BF)


def on_device(queries, keys, values, d_mixed, series_ids, variate_ids, variate_bias, w_out):
    query, key_rows, value_rows, upstream = queries[0], keys[0], values[0], d_mixed[0]
    tok, width = query.shape
    n_ctx, n_dp = lax.axis_size("ctx"), lax.axis_size("dp")
    total, pairs, cols, block = tok * n_ctx, width // PAIR, width // n_ctx, width // n_dp
    me_ctx, me_dp = lax.axis_index("ctx"), lax.axis_index("dp")
    bits = [1 << i for i in range(n_dp.bit_length() - 1)]
    assert 1 << len(bits) == n_dp and n_dp > 1 and n_ctx > 1

    def swap(array, bit):
        return lax.ppermute(array, "dp", [(i, i ^ bit) for i in range(n_dp)])

    def turn(array, by):
        return lax.ppermute(array, "ctx", [(i, (i + by) % n_ctx) for i in range(n_ctx)])

    def others(array, axis):
        parts = [turn(array, by) for by in range(1, n_ctx)]
        return parts[0] if len(parts) == 1 else jnp.concatenate(parts, axis=axis)

    kx = others(key_rows, 0)
    vx = others(value_rows, 0)
    qx = others(query, 0)
    code = series_ids * 256 + variate_ids
    code_x = others(code, 1)
    dx = others(upstream, 0)

    pieces = {0: w_out}
    for bit in reversed(bits):
        for piece in list(pieces):
            pieces[piece ^ bit] = swap(pieces[piece], bit)
    order = list(pieces)
    where = jnp.stack([me_ctx, me_dp % 2, me_dp]).astype(jnp.int32)

    smem = pl.BlockSpec(memory_space=pltpu.SMEM)

    def whole(array):
        return pl.BlockSpec(array.shape, lambda i, *_: (0,) * array.ndim)

    def lane(rows):
        return pl.BlockSpec((rows, PAIR), lambda i, *_: (0, i))

    own, oth, row = lane(tok), lane(total - tok), lane(total)
    w_specs = [pl.BlockSpec((GROUP, tok, total), lambda i, *_: (i, 0, 0)),
               pl.BlockSpec((GROUP, total - tok, tok), lambda i, *_: (i, 0, 0))]
    params = pltpu.CompilerParams(dimension_semantics=("arbitrary",), vmem_limit_bytes=24 << 20)
    ctx, w_own, w_oth = pl.pallas_call(
        forward_kernel,
        grid=(pairs,),
        in_specs=[smem, whole(code), whole(code_x), own, oth, own, oth, own, oth],
        out_specs=[row, *w_specs],
        out_shape=[jax.ShapeDtypeStruct((total, width), F32),
                   jax.ShapeDtypeStruct((HEADS, tok, total), BF),
                   jax.ShapeDtypeStruct((HEADS, total - tok, tok), BF)],
        scratch_shapes=[pltpu.VMEM((total, total), F32), pltpu.VMEM((total, total), F32)],
        compiler_params=params,
        cost_estimate=pl.CostEstimate(flops=4 * HEADS * total * total * HEAD_DIM * 4,
                                      bytes_accessed=8 << 20, transcendentals=HEADS * total * total),
        name="forward",
    )(variate_bias, code, code_x, query, qx, key_rows, kx, value_rows, vx)

    half_spec = lambda rows: pl.BlockSpec((rows, cols), lambda i, where: (0, where[0]))
    keep, send = pl.pallas_call(
        weight_kernel,
        grid_spec=pltpu.PrefetchScalarGridSpec(
            num_scalar_prefetch=1,
            grid=(2,),
            in_specs=[pl.BlockSpec((total, width // 2), lambda i, *_: (0, i)), half_spec(tok),
                      half_spec(total - tok)],
            out_specs=[pl.BlockSpec((n_dp // 4, block, cols), lambda i, *_: (i, 0, 0))] * 2),
        out_shape=[jax.ShapeDtypeStruct((n_dp // 2, block, cols), F32),
                   jax.ShapeDtypeStruct((n_dp // 2, block, cols), BF)],
        compiler_params=params,
        cost_estimate=pl.CostEstimate(flops=2 * total * width * cols, bytes_accessed=4 << 20,
                                      transcendentals=0),
        name="weights",
    )(where, ctx, upstream, dx)

    for bit in bits:
        summed = keep + swap(send, bit).astype(F32)
        if bit != bits[-1]:
            low = (me_dp // (2 * bit)) % 2 == 0
            summed = summed.reshape(-1, 2, block, cols)
            keep = jnp.where(low, summed[:, 0], summed[:, 1])
            send = jnp.where(low, summed[:, 1], summed[:, 0]).astype(BF)
    summed = summed[0]
    sent = summed.astype(BF)
    if n_ctx == 2:
        got = turn(sent, 1).astype(F32)
        first = me_ctx == 0
        w_grad = jnp.concatenate([jnp.where(first, summed, got), jnp.where(first, got, summed)], axis=1)
    else:
        parts = [summed] + [turn(sent, by).astype(F32) for by in range(1, n_ctx)]
        w_grad = jnp.concatenate(
            [sum(jnp.where((me_ctx - by) % n_ctx == c, part, 0.0) for by, part in enumerate(parts))
             for c in range(n_ctx)], axis=1)

    mixed, q_grad, k_grad, v_grad, bias_rows = pl.pallas_call(
        functools.partial(backward_kernel, order),
        grid=(pairs,),
        in_specs=[smem, whole(code), whole(code_x), whole(upstream), whole(dx), own, oth, own, oth,
                  own, oth, row, *w_specs, *[whole(w_out)] * n_dp],
        out_specs=[whole(query), own, own, own, pl.BlockSpec((1, 2 * GROUP, total), lambda i, *_: (i, 0, 0))],
        out_shape=[jax.ShapeDtypeStruct((tok, width), BF)] * 4
        + [jax.ShapeDtypeStruct((pairs, 2 * GROUP, total), F32)],
        scratch_shapes=[pltpu.VMEM((n_dp // 2, 2, block, width), BF), pltpu.VMEM((tok, total), F32),
                        pltpu.VMEM((tok, width), F32), pltpu.VMEM((total, width), BF)],
        compiler_params=params,
        cost_estimate=pl.CostEstimate(flops=10 * HEADS * total * total * HEAD_DIM * 4,
                                      bytes_accessed=10 << 20, transcendentals=0),
        name="backward",
    )(where, code, code_x, upstream, dx, query, qx, key_rows, kx, value_rows, vx, ctx, w_own, w_oth,
      *[pieces[p] for p in order])

    sums = jnp.sum(bias_rows, axis=2)
    for bit in bits:
        sums = sums + swap(sums, bit)
    sums = sum((turn(sums, by) for by in range(1, n_ctx)), sums)
    sums = sums.reshape(pairs, GROUP, 2)
    bias_grad = jnp.stack([sums[:, :, 0].reshape(HEADS), (sums[:, :, 1] - sums[:, :, 0]).reshape(HEADS)])
    return mixed[None], q_grad[None], k_grad[None], v_grad[None], w_grad, bias_grad


def solution(mesh):
    data = P("dp", "ctx", None)

    return jax.shard_map(
        on_device,
        mesh=mesh,
        in_specs=(data, data, data, data, P("dp", "ctx"), P("dp", "ctx"), P(), P("dp", None)),
        out_specs=(data, data, data, data, P("dp", None), P()),
        check_vma=False,
    )
```

```python
import functools

import jax
import jax.numpy as jnp
from jax import lax
from jax.experimental import pallas as pl
from jax.experimental.pallas import tpu as pltpu
from jax.sharding import PartitionSpec as P


HEADS = 16
HEAD_DIM = 64
GROUP = 4
LANES = GROUP * HEAD_DIM
SCALE = HEAD_DIM ** -0.5
NEG = -1e30
TAIL = 16
BF = jnp.bfloat16
F32 = jnp.float32


def dot_nt(a, b):
    return lax.dot_general(a, b, (((1,), (1,)), ((), ())), preferred_element_type=F32)


def dot_tn(a, b):
    return lax.dot_general(a, b, (((0,), (0,)), ((), ())), preferred_element_type=F32)


def dot_nn(a, b):
    return lax.dot_general(a, b, (((1,), (0,)), ((), ())), preferred_element_type=F32)


def both(own_ref, oth_ref):
    return jnp.concatenate([own_ref[...], oth_ref[...]], axis=0)


def columns(row):
    return jnp.transpose(jnp.broadcast_to(row, (128, row.shape[1])))[:, :1]


def low_bit(bit):
    return (lax.axis_index("dp") // bit) % 2 == 0


def prepare_kernel(series_ref, variate_ref, *refs):
    count = (len(refs) - 2) // 2
    sources, code_ref, targets, sem = refs[:count], refs[count], refs[count + 1:-1], refs[-1]
    copies = [pltpu.make_async_copy(source, target, sem.at[i])
              for i, (source, target) in enumerate(zip(sources, targets))]
    for copy in copies:
        copy.start()
    code_ref[...] = series_ref[...] * 256 + variate_ref[...]
    for copy in copies:
        copy.wait()


def each_group(width, body):
    def step(group, carry):
        body(group, pl.ds(pl.multiple_of(group * LANES, LANES), LANES))
        return carry

    lax.fori_loop(0, width // LANES, step, 0)


def forward_kernel(own, bias_ref, ido_ref, idx_ref, q_ref, ko_ref, kx_ref, vo_ref, vx_ref,
                   ctx_ref, w_ref, neg_ref, same_ref):
    count, tok = q_ref.shape[0], ko_ref.shape[0]
    row = jnp.concatenate([ido_ref[...], idx_ref[...]], axis=1)
    col = columns(ido_ref[...] if own else idx_ref[...])
    neg_ref[...] = jnp.where((row >> 8) == (col >> 8), 0.0, NEG)
    same_ref[...] = jnp.where((row & 255) == (col & 255), 1.0, 0.0)

    def body(group, at):
        k = jnp.concatenate([ko_ref[:, at], kx_ref[:, at]], axis=0)
        v = jnp.concatenate([vo_ref[:, at], vx_ref[:, at]], axis=0)
        q = q_ref[:, at] * jnp.asarray(SCALE, BF)
        for start in range(0, count, tok):
            rows = slice(start, start + tok)
            found = []
            for part in range(GROUP):
                head = GROUP * group + part
                gap = bias_ref[0, head] - bias_ref[1, head]
                lanes = slice(part * HEAD_DIM, (part + 1) * HEAD_DIM)
                s = dot_nt(q[rows, lanes], k[:, lanes]) + (same_ref[rows, :] * gap + neg_ref[rows, :])
                e = jnp.exp(s - jnp.max(s, axis=1, keepdims=True))
                w = (e * (1.0 / jnp.sum(e, axis=1, keepdims=True))).astype(BF)
                found.append(dot_nn(w, v[:, lanes]))
                w_ref[head, rows, :] = w if own else w[:, :tok]
            ctx_ref[rows, at] = jnp.concatenate(found, axis=1)

    each_group(ko_ref.shape[1], body)


def split(summed, bit, keep_ref, send_ref):
    n, block, cols = keep_ref.shape
    low = low_bit(bit)
    summed = summed.reshape(n, 2, block, cols)
    keep_ref[...] = jnp.where(low, summed[:, 0], summed[:, 1])
    send = jnp.where(low, summed[:, 1], summed[:, 0]).astype(BF)
    send_ref[:n * block, :] = send.reshape(n * block, cols)


def weight_kernel(co_ref, cx_ref, do_ref, dx_ref, keep_ref, send_ref):
    n, _, cols = keep_ref.shape
    cut = pl.ds(pl.multiple_of(lax.axis_index("ctx") * cols, 128), cols)
    d = jnp.concatenate([do_ref[:, cut], dx_ref[:, cut]], axis=0)
    half = co_ref.shape[1] // 2
    for part in range(2):
        at = slice(part * half, (part + 1) * half)
        c = jnp.concatenate([co_ref[:, at], cx_ref[:, at]], axis=0).astype(BF)
        split(dot_tn(c, d), 1, keep_ref.at[part * n // 2:(part + 1) * n // 2],
              send_ref.at[part * half // 2:(part + 1) * half // 2])


def pack_tail(sums, send_ref):
    rows, cols = send_ref.shape
    high = sums.astype(BF)
    low = (sums - high.astype(F32)).astype(BF)
    place = lax.broadcasted_iota(jnp.int32, (TAIL, 128), 0)
    tail = jnp.where(place == 0, high.astype(F32), jnp.where(place == 1, low.astype(F32), 0.0)).astype(BF)
    send_ref[rows - TAIL:, :128] = tail
    if cols > 128:
        send_ref[rows - TAIL:, 128:] = jnp.zeros((TAIL, cols - 128), BF)


def unpack_tail(got_ref):
    tail = got_ref[got_ref.shape[0] - TAIL:, :128].astype(F32)
    return tail[0:1] + tail[1:2]


def halve_kernel(bit, last, packed, keep_ref, got_ref, *refs):
    n, block, cols = keep_ref.shape
    summed = keep_ref[...] + got_ref[:n * block, :].astype(F32).reshape(n, block, cols)
    refs = list(refs)
    sums = None
    if packed is not None:
        sums = refs.pop(0)[...] + (refs.pop(0)[...] if packed == "apart" else unpack_tail(got_ref))
    out_ref, send_ref = refs[0], refs[1]
    if last:
        out_ref[...] = summed[0]
        send_ref[:block, :] = summed[0].astype(BF)
    else:
        split(summed, bit, out_ref, send_ref)
    if sums is not None:
        pack_tail(sums, send_ref)
        refs[2][...] = sums


def add_kernel(a_ref, b_ref, out_ref):
    out_ref[...] = a_ref[...] + b_ref[...]


def final_kernel(keep_ref, sums_ref, *refs):
    got, (w_ref, bias_ref) = refs[:-2], refs[-2:]
    block, cols = keep_ref.shape
    n, me = lax.axis_size("ctx"), lax.axis_index("ctx")
    sums = sums_ref[...]
    w_ref[:, pl.ds(pl.multiple_of(me * cols, 128), cols)] = keep_ref[...]
    for by, ref in enumerate(got, 1):
        sums = sums + unpack_tail(ref)
        at = pl.multiple_of(((me + n - by) % n) * cols, 128)
        w_ref[:, pl.ds(at, cols)] = ref[:block, :].astype(F32)
    same, total = sums[:, :HEADS], sums[:, HEADS:2 * HEADS]
    bias_ref[0:1, :] = same
    bias_ref[1:2, :] = total - same


def score_grad_kernel(pieces, ido_ref, idx_ref, do_ref, dx_ref, vo_ref, vx_ref, co_ref, cx_ref,
                      wo_ref, wx_ref, *rest):
    piece_refs = rest[:len(pieces)]
    wfull_ref, dc_ref, so_ref, sx_ref, sums_ref, same_ref, rows_ref = rest[len(pieces):]
    tok = vo_ref.shape[0]
    nb = LANES // (2 * wfull_ref.shape[2])
    row = jnp.concatenate([ido_ref[...], idx_ref[...]], axis=1)
    same_ref[...] = jnp.where((row & 255) == (columns(ido_ref[...]) & 255), 1.0, 0.0)
    for piece, ref in zip(pieces, piece_refs):
        index = jnp.bitwise_xor(lax.axis_index("dp"), piece)
        wfull_ref[index // 2, index % 2] = ref[...]

    def body(group, at):
        w = wfull_ref[pl.ds(group * nb, nb)].reshape(LANES, wfull_ref.shape[3])
        d = dot_nt(both(do_ref, dx_ref), w).astype(BF)
        dc_ref[:, at] = d
        prod = d.astype(F32) * jnp.concatenate([co_ref[:, at], cx_ref[:, at]], axis=0)
        v = jnp.concatenate([vo_ref[:, at], vx_ref[:, at]], axis=0)
        same = same_ref[...]
        for part in range(GROUP):
            lanes = slice(part * HEAD_DIM, (part + 1) * HEAD_DIM)
            dh, vh = d[:, lanes], v[:, lanes]
            delta = jnp.sum(prod[:, lanes], axis=1, keepdims=True)
            head = GROUP * group + part
            ds = wo_ref[head].astype(F32) * (dot_nt(dh[:tok], vh) - delta[:tok])
            rows_ref[pl.ds(head, 1), :] = jnp.sum(ds * same, axis=0, keepdims=True)
            rows_ref[pl.ds(HEADS + head, 1), :] = jnp.sum(ds, axis=0, keepdims=True)
            so_ref[head] = ds.astype(BF)
            sx_ref[head] = (wx_ref[head].astype(F32) * (dot_nt(dh[tok:], vh[:tok]) - delta[tok:])).astype(BF)

    each_group(vo_ref.shape[1], body)
    col = jnp.sum(rows_ref[...], axis=1, keepdims=True)
    col = jnp.concatenate([col, jnp.zeros((128 - 2 * HEADS, 1), F32)], axis=0)
    sums_ref[...] = jnp.transpose(jnp.broadcast_to(col, (128, 128)))[:1]


def input_grad_kernel(qo_ref, qx_ref, ko_ref, kx_ref, co_ref, dc_ref, wo_ref, wx_ref, so_ref, sx_ref,
                      wfull_ref, mixed_ref, qg_ref, kg_ref, vg_ref, acc_ref):
    tok = qo_ref.shape[0]
    nb = LANES // (2 * wfull_ref.shape[2])
    acc_ref[...] = jnp.zeros_like(acc_ref)

    def body(group, at):
        w = wfull_ref[pl.ds(group * nb, nb)].reshape(LANES, wfull_ref.shape[3])
        acc_ref[...] += dot_nn(co_ref[:, at].astype(BF), w)
        q = jnp.concatenate([qo_ref[:, at], qx_ref[:, at]], axis=0) * jnp.asarray(SCALE, BF)
        k = jnp.concatenate([ko_ref[:, at], kx_ref[:, at]], axis=0)
        d = dc_ref[:, at]
        found = []
        for part in range(GROUP):
            lanes = slice(part * HEAD_DIM, (part + 1) * HEAD_DIM)
            dh, qh, kh = d[:, lanes], q[:, lanes], k[:, lanes]
            head = GROUP * group + part
            so, sx, wo, wx = so_ref[head], sx_ref[head], wo_ref[head], wx_ref[head]
            found.append((dot_nn(so, kh) * SCALE,
                          dot_tn(so[:, :tok], qh[:tok]) + dot_tn(sx, qh[tok:]),
                          dot_tn(wo[:, :tok], dh[:tok]) + dot_tn(wx, dh[tok:])))
        for ref, parts in zip((qg_ref, kg_ref, vg_ref), zip(*found)):
            ref[:, at] = jnp.concatenate(parts, axis=1).astype(BF)

    each_group(qo_ref.shape[1], body)
    mixed_ref[...] = acc_ref[...].astype(BF)


def shape(dims, dtype):
    return jax.ShapeDtypeStruct(dims, dtype)


def cost(flops):
    return pl.CostEstimate(flops=flops, bytes_accessed=4 << 20, transcendentals=0)


def plain(kernel, args, outs, flops=1 << 22, scratch=(), in_specs=None, limit=8 << 20):
    spec = pl.BlockSpec(memory_space=pltpu.VMEM)
    return pl.pallas_call(
        kernel, in_specs=in_specs or [spec] * len(args), out_specs=[spec] * len(outs), out_shape=outs,
        scratch_shapes=scratch, compiler_params=pltpu.CompilerParams(vmem_limit_bytes=limit),
        cost_estimate=cost(flops))(*args)


def on_device(queries, keys, values, d_mixed, series_ids, variate_ids, variate_bias, w_out):
    query, key_rows, value_rows, upstream = queries[0], keys[0], values[0], d_mixed[0]
    tok, width = query.shape
    n_ctx, n_dp = lax.axis_size("ctx"), lax.axis_size("dp")
    total, cols, block = tok * n_ctx, width // n_ctx, width // n_dp
    rest = total - tok
    bits = [1 << i for i in range(n_dp.bit_length() - 1)]
    assert 1 << len(bits) == n_dp and len(bits) > 3 and n_ctx > 1

    def swap(array, bit):
        return lax.ppermute(array, "dp", [(i, i ^ bit) for i in range(n_dp)])

    def turns(array):
        return [lax.ppermute(array, "ctx", [(i, (i + by) % n_ctx) for i in range(n_ctx)])
                for by in range(1, n_ctx)]

    def others(array, axis):
        parts = turns(array)
        return parts[0] if len(parts) == 1 else jnp.concatenate(parts, axis=axis)

    kx = others(key_rows, 0)
    vx = others(value_rows, 0)
    qx = others(query, 0)
    vmem, smem, hbm = [pl.BlockSpec(memory_space=space) for space in (pltpu.VMEM, pltpu.SMEM, pltpu.HBM)]
    limit = (12 << 20) + 40 * total * width
    local = [query, key_rows, value_rows, upstream]
    code, query, key_rows, value_rows, upstream = plain(
        prepare_kernel, [series_ids, variate_ids, *local],
        [shape(series_ids.shape, jnp.int32)] + [shape(a.shape, BF) for a in local],
        scratch=[pltpu.SemaphoreType.DMA((len(local),))], in_specs=[vmem] * 2 + [hbm] * len(local))
    code_x = others(code, 1)
    dx = others(local[3], 0)

    pieces = {0: w_out}
    for bit in reversed(bits):
        for piece in list(pieces):
            pieces[piece ^ bit] = swap(pieces[piece], bit)
    order = list(pieces)

    o_shape, x_shape = shape((HEADS, tok, total), BF), shape((HEADS, rest, tok), BF)

    def forward(is_own, rows):
        args = [variate_bias, code, code_x, query if is_own else qx, key_rows, kx, value_rows, vx]
        return plain(functools.partial(forward_kernel, is_own), args,
                     [shape((rows, width), F32), o_shape if is_own else x_shape],
                     16 * HEADS * rows * total * HEAD_DIM, [pltpu.VMEM((rows, total), F32)] * 2,
                     [smem] + [vmem] * (len(args) - 1), limit)

    ctx_o, w_o = forward(True, tok)
    ctx_x, w_x = forward(False, rest)
    keep, send = plain(weight_kernel, [ctx_o, ctx_x, upstream, dx],
                       [shape((n_dp // 2, block, cols), F32), shape((width // 2, cols), BF)],
                       2 * total * width * cols, limit=limit)
    w_full, d_ctx, s_o, s_x, sums = plain(
        functools.partial(score_grad_kernel, order),
        [code, code_x, upstream, dx, value_rows, vx, ctx_o, ctx_x, w_o, w_x, *[pieces[p] for p in order]],
        [shape((n_dp // 2, 2, block, width), BF), shape((total, width), BF), o_shape, x_shape,
         shape((1, 128), F32)], 16 * HEADS * total * total * HEAD_DIM,
        [pltpu.VMEM((tok, total), F32), pltpu.VMEM((2 * HEADS, total), F32)], limit=limit)

    early = bits[:2]
    for bit in early:
        got = swap(sums, bit)
        if bit != early[-1]:
            sums, = plain(add_kernel, [sums, got], [shape((1, 128), F32)])
    for bit, after in zip(bits, bits[1:] + [None]):
        got_rows = swap(send, bit)
        n = keep.shape[0]
        packed = None if bit < early[-1] else ("apart" if bit == early[-1] else "joined")
        extra = {None: [], "apart": [sums, got], "joined": [sums]}[packed]
        rows = block if after is None else n // 2 * block
        outs = [shape((block, cols) if after is None else (n // 2, block, cols), F32),
                shape((rows + (TAIL if packed else 0), cols), BF)]
        if packed:
            outs.append(shape((1, 128), F32))
        done = plain(functools.partial(halve_kernel, after, after is None, packed),
                     [keep, got_rows, *extra], outs)
        keep, send = done[:2]
        if packed:
            sums = done[2]
    parts = turns(send)
    w_grad, bias_grad = plain(final_kernel, [keep, sums, *parts],
                              [shape((block, width), F32), shape((2, HEADS), F32)])
    mixed, q_grad, k_grad, v_grad = plain(
        input_grad_kernel, [query, qx, key_rows, kx, ctx_o, d_ctx, w_o, w_x, s_o, s_x, w_full],
        [shape((tok, width), BF)] * 4, 16 * HEADS * total * total * HEAD_DIM,
        [pltpu.VMEM((tok, width), F32)], limit=limit)
    return mixed[None], q_grad[None], k_grad[None], v_grad[None], w_grad, bias_grad


def solution(mesh):
    data = P("dp", "ctx", None)

    return jax.shard_map(
        on_device,
        mesh=mesh,
        in_specs=(data, data, data, data, P("dp", "ctx"), P("dp", "ctx"), P(), P("dp", None)),
        out_specs=(data, data, data, data, P("dp", None), P()),
        check_vma=False,
    )
```

```python
import functools

import jax
import jax.numpy as jnp
from jax import lax
from jax.experimental import pallas as pl
from jax.experimental.pallas import tpu as pltpu
from jax.sharding import PartitionSpec as P


HEADS = 16
HEAD_DIM = 64
PAIR = 2 * HEAD_DIM
SCALE = HEAD_DIM ** -0.5
NEG = -1e30
TAIL = 16
BF = jnp.bfloat16
F32 = jnp.float32


def dot_nt(a, b):
    return lax.dot_general(a, b, (((1,), (1,)), ((), ())), preferred_element_type=F32)


def dot_tn(a, b):
    return lax.dot_general(a, b, (((0,), (0,)), ((), ())), preferred_element_type=F32)


def dot_nn(a, b):
    return lax.dot_general(a, b, (((1,), (0,)), ((), ())), preferred_element_type=F32)


def columns(row):
    return jnp.transpose(jnp.broadcast_to(row, (128, row.shape[1])))[:, :1]


def low_bit(bit):
    return (lax.axis_index("dp") // bit) % 2 == 0


def prepare_kernel(bias_ref, series_ref, variate_ref, d_ref, q_ref, k_ref, v_ref, code_ref, gap_ref, d_out,
                   qv_out, k_out, *refs):
    cuts, (bias_buf, ids_ref, sem) = refs[:-3], refs[-3:]
    tok = d_ref.shape[0]
    moves = [(bias_ref, bias_buf), (series_ref, ids_ref.at[0]), (variate_ref, ids_ref.at[1]), (d_ref, d_out),
             (q_ref, qv_out.at[:tok]), (v_ref, qv_out.at[tok:]), (k_ref, k_out)]
    copies = [pltpu.make_async_copy(source, target, sem.at[i]) for i, (source, target) in enumerate(moves)]
    for copy in copies:
        copy.start()
    for copy in copies:
        copy.wait()
    code_ref[...] = ids_ref[0] * 256 + ids_ref[1]
    gap = jnp.broadcast_to(bias_buf[0:1, :] - bias_buf[1:2, :], (128, HEADS))
    gap = jnp.concatenate([gap, jnp.zeros((128, 128 - HEADS), F32)], axis=1)
    gap_ref[...] = jnp.transpose(gap)[:HEADS]
    n, me, cols = lax.axis_size("ctx"), lax.axis_index("ctx"), cuts[0].shape[1]
    for by, ref in enumerate(cuts, 1):
        ref[...] = d_out[:, pl.ds(pl.multiple_of(((me + by) % n) * cols, 128), cols)]


def heads_at_once(tokens):
    return HEADS if tokens <= 512 else 4


def each_group(tokens, body):
    group = heads_at_once(tokens)
    lanes = group * HEAD_DIM
    if group == HEADS:
        body(0, slice(0, lanes))
        return

    def step(index, carry):
        body(index, pl.ds(pl.multiple_of(index * lanes, lanes), lanes))
        return carry

    lax.fori_loop(0, HEADS // group, step, 0)


def low_lanes(rows):
    return lax.broadcasted_iota(jnp.int32, (rows, PAIR), 1) < HEAD_DIM


def stacked(pair):
    low, zero = low_lanes(pair.shape[0]), jnp.zeros_like(pair)
    return jnp.concatenate([jnp.where(low, pair, zero), jnp.where(low, zero, pair)], axis=0)


def unstacked(rows):
    half = rows.shape[0] // 2
    return jnp.where(low_lanes(half), rows[:half], rows[half:])


def equal_ids(own_ref, oth_ref, count, shift):
    row = (jnp.concatenate([own_ref[...], oth_ref[...]], axis=1) >> shift) & 255
    return row == columns(row)[:count]


def forward_kernel(gap_ref, ido_ref, idx_ref, qvo_ref, qvx_ref, ko_ref, kx_ref,
                   co_ref, cx_ref, wo_ref, wx_ref, neg_ref, same_ref):
    tok, rest = co_ref.shape[0], cx_ref.shape[0]
    heads = heads_at_once(tok + rest)
    neg_ref[...] = jnp.where(equal_ids(ido_ref, idx_ref, tok + rest, 8), 0.0, NEG)
    same_ref[...] = jnp.where(equal_ids(ido_ref, idx_ref, tok + rest, 0), 1.0, 0.0)

    def body(group, at):
        k = jnp.concatenate([ko_ref[:, at], kx_ref[:, at]], axis=0)
        v = jnp.concatenate([qvo_ref[tok:, at], qvx_ref[rest:, at]], axis=0)
        for chunk in range((tok + rest) // tok):
            rows = slice(chunk * tok, (chunk + 1) * tok)
            place = slice((chunk - 1) * tok, chunk * tok)
            q = (qvx_ref[place, at] if chunk else qvo_ref[:tok, at]) * jnp.asarray(SCALE, BF)
            found = []
            for pair in range(heads // 2):
                lanes = slice(pair * PAIR, (pair + 1) * PAIR)
                s = dot_nt(stacked(q[:, lanes]), k[:, lanes])
                both_w = []
                for half in range(2):
                    head = heads * group + 2 * pair + half
                    gap = gap_ref[pl.ds(head, 1), :1]
                    sh = s[half * tok:(half + 1) * tok] + (same_ref[rows, :] * gap + neg_ref[rows, :])
                    e = jnp.exp(sh - jnp.max(sh, axis=1, keepdims=True))
                    w = (e * (1.0 / jnp.sum(e, axis=1, keepdims=True))).astype(BF)
                    if chunk:
                        wx_ref[head, place, :] = w[:, :tok]
                    else:
                        wo_ref[head] = w
                    both_w.append(w)
                found.append(unstacked(dot_nn(jnp.concatenate(both_w, axis=0), v[:, lanes])))
            if chunk:
                cx_ref[place, at] = jnp.concatenate(found, axis=1)
            else:
                co_ref[:, at] = jnp.concatenate(found, axis=1)

    each_group(tok + rest, body)


def split(summed, bit, keep_ref, send_ref, low=1):
    n, block, cols = keep_ref.shape
    mine = low_bit(bit)
    summed = summed.reshape(n // low, 2, low, block, cols)
    keep = jnp.where(mine, summed[:, 0], summed[:, 1])
    send = jnp.where(mine, summed[:, 1], summed[:, 0])
    keep_ref[...] = keep.reshape(n, block, cols)
    write_blocks(send.reshape(n * block, cols), send_ref)


def write_blocks(rows, send_ref):
    count, lanes = rows.shape[0], send_ref.shape[1]
    for part in range(rows.shape[1] // lanes):
        send_ref[part * count:(part + 1) * count, :] = rows[:, part * lanes:(part + 1) * lanes].astype(BF)


def read_blocks(got_ref, count, cols):
    lanes = got_ref.shape[1]
    parts = [got_ref[part * count:(part + 1) * count, :].astype(F32) for part in range(cols // lanes)]
    return jnp.concatenate(parts, axis=1)


def weight_kernel(co_ref, cx_ref, do_ref, dx_ref, keep_ref, send_ref):
    n, _, cols = keep_ref.shape
    cut = pl.ds(pl.multiple_of(lax.axis_index("ctx") * cols, 128), cols)
    d = jnp.concatenate([do_ref[:, cut], dx_ref[...]], axis=0)
    half = co_ref.shape[1] // 2
    for part in range(2):
        at = slice(part * half, (part + 1) * half)
        c = jnp.concatenate([co_ref[:, at], cx_ref[:, at]], axis=0).astype(BF)
        split(dot_tn(c, d), 1, keep_ref.at[part * n // 2:(part + 1) * n // 2],
              send_ref.at[part * half // 2:(part + 1) * half // 2])


def pack_tail(sums, send_ref):
    high = sums.astype(BF)
    low = (sums - high.astype(F32)).astype(BF)
    place = lax.broadcasted_iota(jnp.int32, (TAIL, 128), 0)
    tail = jnp.where(place == 0, high.astype(F32), jnp.where(place == 1, low.astype(F32), 0.0))
    send_ref[send_ref.shape[0] - TAIL:, :] = tail.astype(BF)


def unpack_tail(got_ref):
    tail = got_ref[got_ref.shape[0] - TAIL:, :].astype(F32)
    return tail[0:1] + tail[1:2]


def halve_kernel(bit, low, keep_ref, got_ref, *refs):
    n, block, cols = keep_ref.shape
    summed = keep_ref[...] + got_ref[...].astype(F32).reshape(n, block, cols)
    if len(refs) == 2:
        split(summed, bit, *refs, low=low)
        return
    sums_ref, extra_ref, keep_out, send_ref, keep_send_ref, sums_out = refs
    split(summed, bit, keep_out, send_ref)
    write_blocks(keep_out[0], keep_send_ref)
    sums = sums_ref[...] + extra_ref[...]
    sums_out[...] = sums
    pack_tail(sums, send_ref)
    pack_tail(sums, keep_send_ref)


def add_kernel(a_ref, b_ref, out_ref):
    out_ref[...] = a_ref[...] + b_ref[...]


def final_kernel(keep_ref, sums_ref, got_ref, *refs):
    got, (w_ref, bias_ref) = refs[:-2], refs[-2:]
    _, block, cols = keep_ref.shape
    n, me = lax.axis_size("ctx"), lax.axis_index("ctx")
    sums = sums_ref[...] + unpack_tail(got_ref)
    w_ref[:, pl.ds(pl.multiple_of(me * cols, 128), cols)] = keep_ref[0] + read_blocks(got_ref, block, cols)
    for by, (ref, more_ref) in enumerate(zip(got[::2], got[1::2]), 1):
        sums = sums + (unpack_tail(ref) + unpack_tail(more_ref))
        at = pl.multiple_of(((me + n - by) % n) * cols, 128)
        w_ref[:, pl.ds(at, cols)] = read_blocks(ref, block, cols) + read_blocks(more_ref, block, cols)
    same, total = sums[:, :HEADS], sums[:, HEADS:2 * HEADS]
    bias_ref[0:1, :] = same
    bias_ref[1:2, :] = total - same


def score_grad_kernel(pieces, parts, ido_ref, idx_ref, qvo_ref, qvx_ref, co_ref, cx_ref, wo_ref, wx_ref,
                      do_ref, *rest):
    dx_refs, piece_refs = rest[:parts], rest[parts:parts + len(pieces)]
    wfull_ref, dc_ref, so_ref, sx_ref, sums_ref, same_ref, dall_ref, rows_ref = rest[parts + len(pieces):]
    tok, rest_rows = qvo_ref.shape[0] // 2, qvx_ref.shape[0] // 2
    heads = heads_at_once(tok + rest_rows)
    nb = heads * HEAD_DIM // (2 * wfull_ref.shape[2])
    same_ref[...] = jnp.where(equal_ids(ido_ref, idx_ref, tok, 0), 1.0, 0.0)
    dall_ref[:tok, :] = do_ref[...]
    if parts == 1:
        dall_ref[tok:, :] = dx_refs[0][...]
    else:
        me, cols = lax.axis_index("ctx"), dx_refs[0].shape[1]
        for ref, at in zip(dx_refs, (me, 1 - me)):
            dall_ref[tok:, pl.ds(pl.multiple_of(at * cols, 128), cols)] = ref[...]
    for piece, ref in zip(pieces, piece_refs):
        index = jnp.bitwise_xor(lax.axis_index("dp"), piece)
        wfull_ref[index // 2, index % 2] = ref[...]

    def body(group, at):
        w = wfull_ref[pl.ds(group * nb, nb)].reshape(heads * HEAD_DIM, wfull_ref.shape[3])
        d = dot_nt(dall_ref[...], w).astype(BF)
        dc_ref[:, at] = d
        prod = d.astype(F32) * jnp.concatenate([co_ref[:, at], cx_ref[:, at]], axis=0)
        v = jnp.concatenate([qvo_ref[tok:, at], qvx_ref[rest_rows:, at]], axis=0)
        same = same_ref[...]
        for pair in range(heads // 2):
            lanes = slice(pair * PAIR, (pair + 1) * PAIR)
            dp, vp = d[:, lanes], v[:, lanes]
            delta = jnp.sum(stacked(prod[:, lanes]), axis=1, keepdims=True)
            total = dp.shape[0]
            own = dot_nt(stacked(dp[:tok]), vp)
            oth = dot_nt(stacked(dp[tok:]), vp[:tok])
            for half in range(2):
                head = heads * group + 2 * pair + half
                dh = delta[half * total:(half + 1) * total]
                ds = wo_ref[head].astype(F32) * (own[half * tok:(half + 1) * tok] - dh[:tok])
                rows_ref[pl.ds(head, 1), :] = jnp.sum(ds * same, axis=0, keepdims=True)
                rows_ref[pl.ds(HEADS + head, 1), :] = jnp.sum(ds, axis=0, keepdims=True)
                so_ref[head] = ds.astype(BF)
                down = oth[half * rest_rows:(half + 1) * rest_rows]
                sx_ref[head] = (wx_ref[head].astype(F32) * (down - dh[tok:])).astype(BF)

    each_group(tok + rest_rows, body)
    col = jnp.sum(rows_ref[...], axis=1, keepdims=True)
    col = jnp.concatenate([col, jnp.zeros((128 - 2 * HEADS, 1), F32)], axis=0)
    sums_ref[...] = jnp.transpose(jnp.broadcast_to(col, (128, 128)))[:1]


def input_grad_kernel(qvo_ref, qvx_ref, ko_ref, kx_ref, co_ref, dc_ref, wo_ref, wx_ref, so_ref, sx_ref,
                      wfull_ref, mixed_ref, qg_ref, kg_ref, vg_ref, acc_ref):
    tok, rest_rows = qvo_ref.shape[0] // 2, qvx_ref.shape[0] // 2
    heads = heads_at_once(tok + rest_rows)
    nb = heads * HEAD_DIM // (2 * wfull_ref.shape[2])
    acc_ref[...] = jnp.zeros_like(acc_ref)

    def side_by_side(own_ref, oth_ref, head):
        return jnp.concatenate(
            [jnp.concatenate([own_ref[h, :, :tok], oth_ref[h]], axis=0) for h in (head, head + 1)], axis=1)

    def body(group, at):
        w = wfull_ref[pl.ds(group * nb, nb)].reshape(heads * HEAD_DIM, wfull_ref.shape[3])
        acc_ref[...] += dot_nn(co_ref[:, at].astype(BF), w)
        q = jnp.concatenate([qvo_ref[:tok, at], qvx_ref[:rest_rows, at]], axis=0) * jnp.asarray(SCALE, BF)
        k = jnp.concatenate([ko_ref[:, at], kx_ref[:, at]], axis=0)
        d = dc_ref[:, at]
        found = []
        for pair in range(heads // 2):
            lanes = slice(pair * PAIR, (pair + 1) * PAIR)
            head = heads * group + 2 * pair
            so = jnp.concatenate([so_ref[head], so_ref[head + 1]], axis=0)
            found.append((unstacked(dot_nn(so, k[:, lanes])) * SCALE,
                          unstacked(dot_tn(side_by_side(so_ref, sx_ref, head), q[:, lanes])),
                          unstacked(dot_tn(side_by_side(wo_ref, wx_ref, head), d[:, lanes]))))
        for ref, parts in zip((qg_ref, kg_ref, vg_ref), zip(*found)):
            ref[:, at] = jnp.concatenate(parts, axis=1).astype(BF)

    each_group(tok + rest_rows, body)
    mixed_ref[...] = acc_ref[...].astype(BF)


def shape(dims, dtype):
    return jax.ShapeDtypeStruct(dims, dtype)


def cost(flops):
    return pl.CostEstimate(flops=flops, bytes_accessed=4 << 20, transcendentals=0)


def plain(kernel, args, outs, flops=1 << 22, scratch=(), in_specs=None, limit=8 << 20):
    spec = pl.BlockSpec(memory_space=pltpu.VMEM)
    return pl.pallas_call(
        kernel, in_specs=in_specs or [spec] * len(args), out_specs=[spec] * len(outs), out_shape=outs,
        scratch_shapes=scratch, compiler_params=pltpu.CompilerParams(vmem_limit_bytes=limit),
        cost_estimate=cost(flops))(*args)


def on_device(queries, keys, values, d_mixed, series_ids, variate_ids, variate_bias, w_out):
    query, key_rows, value_rows, upstream = queries[0], keys[0], values[0], d_mixed[0]
    tok, width = query.shape
    n_ctx, n_dp = lax.axis_size("ctx"), lax.axis_size("dp")
    total, cols, block = tok * n_ctx, width // n_ctx, width // n_dp
    rest = total - tok
    bits = [1 << i for i in range(n_dp.bit_length() - 1)]
    assert 1 << len(bits) == n_dp and len(bits) > 3 and n_ctx > 1

    def swap(array, bit):
        return lax.ppermute(array, "dp", [(i, i ^ bit) for i in range(n_dp)])

    def turns(array):
        return [lax.ppermute(array, "ctx", [(i, (i + by) % n_ctx) for i in range(n_ctx)])
                for by in range(1, n_ctx)]

    def others(array, axis):
        parts = turns(array)
        return parts[0] if len(parts) == 1 else jnp.concatenate(parts, axis=axis)

    hbm = pl.BlockSpec(memory_space=pltpu.HBM)
    limit = (12 << 20) + 40 * total * width
    kx = others(key_rows, 0)
    local = [variate_bias, series_ids, variate_ids, upstream, query, key_rows, value_rows]
    cut = shape((tok, cols), BF)
    code, gaps, upstream, qv, key_rows, *cuts = plain(
        prepare_kernel, [pltpu.with_memory_space_constraint(a, pltpu.HBM) for a in local],
        [shape(series_ids.shape, jnp.int32), shape((HEADS, 128), F32), shape((tok, width), BF),
         shape((2 * tok, width), BF), shape((tok, width), BF)] + [cut] * n_ctx,
        scratch=[pltpu.VMEM((2, HEADS), F32), pltpu.VMEM((2, 1, tok), jnp.int32), pltpu.SemaphoreType.DMA((len(local),))],
        in_specs=[hbm] * len(local))
    code_x = others(code, 1)
    parts = turns(qv)
    qvx = parts[0] if n_ctx == 2 else jnp.concatenate([p[:tok] for p in parts] + [p[tok:] for p in parts])
    near = [lax.ppermute(part, "ctx", [(i, (i + by) % n_ctx) for i in range(n_ctx)])
            for by, part in enumerate(cuts[:-1], 1)]
    near = near[0] if len(near) == 1 else jnp.concatenate(near, axis=0)
    dx = [near, *turns(cuts[-1])] if n_ctx == 2 else [others(upstream, 0)]

    pieces = {0: w_out}
    for bit in reversed(bits):
        for piece in list(pieces):
            pieces[piece ^ bit] = swap(pieces[piece], bit)
    order = list(pieces)

    o_shape, x_shape = shape((HEADS, tok, total), BF), shape((HEADS, rest, tok), BF)

    ctx_o, ctx_x, w_o, w_x = plain(
        forward_kernel, [gaps, code, code_x, qv, qvx, key_rows, kx],
        [shape((tok, width), F32), shape((rest, width), F32), o_shape, x_shape],
        16 * HEADS * total * total * HEAD_DIM, [pltpu.VMEM((total, total), F32)] * 2, limit=limit)
    keep, send = plain(weight_kernel, [ctx_o, ctx_x, upstream, near],
                       [shape((n_dp // 2, block, cols), F32), shape((width // 2, cols), BF)],
                       2 * total * width * cols, limit=limit)
    w_full, d_ctx, s_o, s_x, sums = plain(
        functools.partial(score_grad_kernel, order, len(dx)),
        [code, code_x, qv, qvx, ctx_o, ctx_x, w_o, w_x, upstream, *dx, *[pieces[p] for p in order]],
        [shape((n_dp // 2, 2, block, width), BF), shape((total, width), BF), o_shape, x_shape,
         shape((1, 128), F32)], 16 * HEADS * total * total * HEAD_DIM,
        [pltpu.VMEM((tok, total), F32), pltpu.VMEM((total, width), BF), pltpu.VMEM((2 * HEADS, total), F32)],
        limit=limit)

    bits = bits[:2] + bits[:1:-1]
    for bit in bits[:-1]:
        got = swap(sums, bit)
        if bit != bits[-2]:
            sums, = plain(add_kernel, [sums, got], [shape((1, 128), F32)])
    for bit, after in zip(bits, bits[1:]):
        n = keep.shape[0] // 2
        args, outs = [keep, swap(send, bit)], [shape((n, block, cols), F32)]
        if n > 1:
            outs.append(shape((n * block, cols), BF))
        else:
            args += [sums, got]
            outs += [shape((block * cols // 128 + TAIL, 128), BF)] * 2 + [shape((1, 128), F32)]
        keep, send, *last = plain(functools.partial(halve_kernel, after, n if after in bits[2:] else 1), args, outs)
    keep_send, sums = last
    args = [keep, sums, swap(send, bits[-1])]
    for by, part in enumerate(turns(keep_send), 1):
        route = [(c * n_dp + d, (c + by) % n_ctx * n_dp + (d ^ bits[-1])) for c in range(n_ctx) for d in range(n_dp)]
        args += [part, lax.ppermute(send, ("ctx", "dp"), route)]
    w_grad, bias_grad = plain(final_kernel, args, [shape((block, width), F32), shape((2, HEADS), F32)])
    mixed, q_grad, k_grad, v_grad = plain(
        input_grad_kernel, [qv, qvx, key_rows, kx, ctx_o, d_ctx, w_o, w_x, s_o, s_x, w_full],
        [shape((tok, width), BF)] * 4, 16 * HEADS * total * total * HEAD_DIM,
        [pltpu.VMEM((tok, width), F32)], limit=limit)
    return mixed[None], q_grad[None], k_grad[None], v_grad[None], w_grad, bias_grad


def solution(mesh):
    data = P("dp", "ctx", None)

    return jax.shard_map(
        on_device,
        mesh=mesh,
        in_specs=(data, data, data, data, P("dp", "ctx"), P("dp", "ctx"), P(), P("dp", None)),
        out_specs=(data, data, data, data, P("dp", None), P()),
        check_vma=False,
    )
```

```python
import functools

import jax
import jax.numpy as jnp
from jax import lax
from jax.experimental import pallas as pl
from jax.experimental.pallas import tpu as pltpu
from jax.sharding import PartitionSpec as P


HEADS = 16
HEAD_DIM = 64
PAIR = 2 * HEAD_DIM
SCALE = HEAD_DIM ** -0.5
NEG = -1e30
TAIL = 16
BF = jnp.bfloat16
F32 = jnp.float32


def dot_nt(a, b):
    return lax.dot_general(a, b, (((1,), (1,)), ((), ())), preferred_element_type=F32)


def dot_tn(a, b):
    return lax.dot_general(a, b, (((0,), (0,)), ((), ())), preferred_element_type=F32)


def dot_nn(a, b):
    return lax.dot_general(a, b, (((1,), (0,)), ((), ())), preferred_element_type=F32)


def columns(row):
    return jnp.transpose(jnp.broadcast_to(row, (128, row.shape[1])))[:, :1]


def low_bit(bit):
    return (lax.axis_index("dp") // bit) % 2 == 0


def prepare_kernel(bias_ref, series_ref, variate_ref, d_ref, q_ref, k_ref, v_ref, code_ref, gap_ref, d_out,
                   qv_out, k_out, *refs):
    cuts, (bias_buf, ids_ref, sem) = refs[:-3], refs[-3:]
    tok = d_ref.shape[0]
    moves = [(bias_ref, bias_buf), (series_ref, ids_ref.at[0]), (variate_ref, ids_ref.at[1]), (d_ref, d_out),
             (q_ref, qv_out.at[:tok]), (v_ref, qv_out.at[tok:]), (k_ref, k_out)]
    copies = [pltpu.make_async_copy(source, target, sem.at[i]) for i, (source, target) in enumerate(moves)]
    for copy in copies:
        copy.start()
    for copy in copies:
        copy.wait()
    code_ref[...] = ids_ref[0] * 256 + ids_ref[1]
    gap = jnp.broadcast_to(bias_buf[0:1, :] - bias_buf[1:2, :], (128, HEADS))
    gap = jnp.concatenate([gap, jnp.zeros((128, 128 - HEADS), F32)], axis=1)
    gap_ref[...] = jnp.transpose(gap)[:HEADS]
    n, me, cols = lax.axis_size("ctx"), lax.axis_index("ctx"), cuts[0].shape[1]
    for by, ref in enumerate(cuts, 1):
        ref[...] = d_out[:, pl.ds(pl.multiple_of(((me + by) % n) * cols, 128), cols)]


def heads_at_once(tokens):
    return HEADS if tokens <= 512 else 4


def each_group(tokens, body):
    group = heads_at_once(tokens)
    lanes = group * HEAD_DIM
    if group == HEADS:
        body(0, slice(0, lanes))
        return

    def step(index, carry):
        body(index, pl.ds(pl.multiple_of(index * lanes, lanes), lanes))
        return carry

    lax.fori_loop(0, HEADS // group, step, 0)


def low_lanes(rows):
    return lax.broadcasted_iota(jnp.int32, (rows, PAIR), 1) < HEAD_DIM


def stacked(pair):
    low, zero = low_lanes(pair.shape[0]), jnp.zeros_like(pair)
    return jnp.concatenate([jnp.where(low, pair, zero), jnp.where(low, zero, pair)], axis=0)


def unstacked(rows):
    half = rows.shape[0] // 2
    return jnp.where(low_lanes(half), rows[:half], rows[half:])


def equal_ids(own_ref, oth_ref, count, shift):
    row = (jnp.concatenate([own_ref[...], oth_ref[...]], axis=1) >> shift) & 255
    return row == columns(row)[:count]


def forward_kernel(gap_ref, ido_ref, idx_ref, qvo_ref, qvx_ref, ko_ref, kx_ref,
                   co_ref, cx_ref, wo_ref, wx_ref, neg_ref, same_ref):
    tok, rest = co_ref.shape[0], cx_ref.shape[0]
    heads = heads_at_once(tok + rest)
    neg_ref[...] = jnp.where(equal_ids(ido_ref, idx_ref, tok + rest, 8), 0.0, NEG)
    same_ref[...] = jnp.where(equal_ids(ido_ref, idx_ref, tok + rest, 0), 1.0, 0.0)

    def body(group, at):
        k = jnp.concatenate([ko_ref[:, at], kx_ref[:, at]], axis=0)
        v = jnp.concatenate([qvo_ref[tok:, at], qvx_ref[rest:, at]], axis=0)
        for chunk in range((tok + rest) // tok):
            rows = slice(chunk * tok, (chunk + 1) * tok)
            place = slice((chunk - 1) * tok, chunk * tok)
            q = (qvx_ref[place, at] if chunk else qvo_ref[:tok, at]) * jnp.asarray(SCALE, BF)
            found = []
            for pair in range(heads // 2):
                lanes = slice(pair * PAIR, (pair + 1) * PAIR)
                s = dot_nt(stacked(q[:, lanes]), k[:, lanes])
                both_w = []
                for half in range(2):
                    head = heads * group + 2 * pair + half
                    gap = gap_ref[pl.ds(head, 1), :1]
                    sh = s[half * tok:(half + 1) * tok] + (same_ref[rows, :] * gap + neg_ref[rows, :])
                    e = jnp.exp(sh - jnp.max(sh, axis=1, keepdims=True))
                    w = (e * (1.0 / jnp.sum(e, axis=1, keepdims=True))).astype(BF)
                    if chunk:
                        wx_ref[head, place, :] = w[:, :tok]
                    else:
                        wo_ref[head] = w
                    both_w.append(w)
                found.append(unstacked(dot_nn(jnp.concatenate(both_w, axis=0), v[:, lanes])))
            if chunk:
                cx_ref[place, at] = jnp.concatenate(found, axis=1)
            else:
                co_ref[:, at] = jnp.concatenate(found, axis=1)

    each_group(tok + rest, body)


def split(summed, bit, keep_ref, send_ref, low=1):
    n, block, cols = keep_ref.shape
    mine = low_bit(bit)
    summed = summed.reshape(n // low, 2, low, block, cols)
    keep = jnp.where(mine, summed[:, 0], summed[:, 1])
    send = jnp.where(mine, summed[:, 1], summed[:, 0])
    keep_ref[...] = keep.reshape(n, block, cols)
    write_blocks(send.reshape(n * block, cols), send_ref)


def write_blocks(rows, send_ref):
    count, lanes = rows.shape[0], send_ref.shape[1]
    for part in range(rows.shape[1] // lanes):
        send_ref[part * count:(part + 1) * count, :] = rows[:, part * lanes:(part + 1) * lanes].astype(BF)


def read_blocks(got_ref, count, cols):
    lanes = got_ref.shape[1]
    parts = [got_ref[part * count:(part + 1) * count, :].astype(F32) for part in range(cols // lanes)]
    return jnp.concatenate(parts, axis=1)


def weight_kernel(co_ref, cx_ref, do_ref, dx_ref, go_ref, stay_ref, send_go_ref, send_stay_ref):
    n, block, cols = go_ref.shape
    cut = pl.ds(pl.multiple_of(lax.axis_index("ctx") * cols, 128), cols)
    d = jnp.concatenate([do_ref[:, cut], dx_ref[...]], axis=0)
    half, some = co_ref.shape[1] // 2, n // 2
    first, second = low_bit(1), low_bit(2)
    for part in range(2):
        at = slice(part * half, (part + 1) * half)
        c = jnp.concatenate([co_ref[:, at], cx_ref[:, at]], axis=0).astype(BF)
        grads = dot_tn(c, d).reshape(some, 2, 2, block, cols)
        kept = jnp.where(first, grads[:, :, 0], grads[:, :, 1])
        sent = jnp.where(first, grads[:, :, 1], grads[:, :, 0])
        rows, place = slice(part * some * block, (part + 1) * some * block), slice(part * some, (part + 1) * some)
        go_ref[place] = jnp.where(second, kept[:, 1], kept[:, 0])
        stay_ref[place] = jnp.where(second, kept[:, 0], kept[:, 1])
        for ref, value in ((send_go_ref, jnp.where(second, sent[:, 1], sent[:, 0])),
                           (send_stay_ref, jnp.where(second, sent[:, 0], sent[:, 1]))):
            ref[rows, :] = value.astype(BF).reshape(some * block, cols)


def sum_kernel(keep_ref, got_ref, out_ref):
    n, block, cols = keep_ref.shape
    summed = keep_ref[...] + got_ref[...].astype(F32).reshape(n, block, cols)
    out_ref[...] = summed.reshape(out_ref.shape).astype(out_ref.dtype)


def pack_tail(sums, send_ref):
    high = sums.astype(BF)
    low = (sums - high.astype(F32)).astype(BF)
    place = lax.broadcasted_iota(jnp.int32, (TAIL, 128), 0)
    tail = jnp.where(place == 0, high.astype(F32), jnp.where(place == 1, low.astype(F32), 0.0))
    send_ref[send_ref.shape[0] - TAIL:, :] = tail.astype(BF)


def unpack_tail(got_ref):
    tail = got_ref[got_ref.shape[0] - TAIL:, :].astype(F32)
    return tail[0:1] + tail[1:2]


def halve_kernel(bit, low, keep_ref, got_ref, *refs):
    n, block, cols = keep_ref.shape
    summed = keep_ref[...] + got_ref[...].astype(F32).reshape(n, block, cols)
    if len(refs) == 2:
        split(summed, bit, *refs, low=low)
        return
    sums_ref, extra_ref, keep_out, send_ref, keep_send_ref, sums_out = refs
    split(summed, bit, keep_out, send_ref)
    write_blocks(keep_out[0], keep_send_ref)
    sums = sums_ref[...] + extra_ref[...]
    sums_out[...] = sums
    pack_tail(sums, send_ref)
    pack_tail(sums, keep_send_ref)


def add_kernel(a_ref, b_ref, out_ref):
    out_ref[...] = a_ref[...] + b_ref[...]


def final_kernel(keep_ref, sums_ref, got_ref, *refs):
    got, (w_ref, bias_ref) = refs[:-2], refs[-2:]
    _, block, cols = keep_ref.shape
    n, me = lax.axis_size("ctx"), lax.axis_index("ctx")
    sums = sums_ref[...] + unpack_tail(got_ref)
    w_ref[:, pl.ds(pl.multiple_of(me * cols, 128), cols)] = keep_ref[0] + read_blocks(got_ref, block, cols)
    for by, (ref, more_ref) in enumerate(zip(got[::2], got[1::2]), 1):
        sums = sums + (unpack_tail(ref) + unpack_tail(more_ref))
        at = pl.multiple_of(((me + n - by) % n) * cols, 128)
        w_ref[:, pl.ds(at, cols)] = read_blocks(ref, block, cols) + read_blocks(more_ref, block, cols)
    same, total = sums[:, :HEADS], sums[:, HEADS:2 * HEADS]
    bias_ref[0:1, :] = same
    bias_ref[1:2, :] = total - same


def score_grad_kernel(pieces, parts, ido_ref, idx_ref, qvo_ref, qvx_ref, co_ref, cx_ref, wo_ref, wx_ref,
                      do_ref, *rest):
    dx_refs, piece_refs = rest[:parts], rest[parts:parts + len(pieces)]
    wfull_ref, dc_ref, so_ref, sx_ref, sums_ref, same_ref, dall_ref, rows_ref = rest[parts + len(pieces):]
    tok, rest_rows = qvo_ref.shape[0] // 2, qvx_ref.shape[0] // 2
    heads = heads_at_once(tok + rest_rows)
    nb = heads * HEAD_DIM // (2 * wfull_ref.shape[2])
    same_ref[...] = jnp.where(equal_ids(ido_ref, idx_ref, tok, 0), 1.0, 0.0)
    dall_ref[:tok, :] = do_ref[...]
    if parts == 1:
        dall_ref[tok:, :] = dx_refs[0][...]
    else:
        me, cols = lax.axis_index("ctx"), dx_refs[0].shape[1]
        for ref, at in zip(dx_refs, (me, 1 - me)):
            dall_ref[tok:, pl.ds(pl.multiple_of(at * cols, 128), cols)] = ref[...]
    for piece, ref in zip(pieces, piece_refs):
        index = jnp.bitwise_xor(lax.axis_index("dp"), piece)
        wfull_ref[index // 2, index % 2] = ref[...]

    def body(group, at):
        w = wfull_ref[pl.ds(group * nb, nb)].reshape(heads * HEAD_DIM, wfull_ref.shape[3])
        d = dot_nt(dall_ref[...], w).astype(BF)
        dc_ref[:, at] = d
        prod = d.astype(F32) * jnp.concatenate([co_ref[:, at], cx_ref[:, at]], axis=0)
        v = jnp.concatenate([qvo_ref[tok:, at], qvx_ref[rest_rows:, at]], axis=0)
        same = same_ref[...]
        for pair in range(heads // 2):
            lanes = slice(pair * PAIR, (pair + 1) * PAIR)
            dp, vp = d[:, lanes], v[:, lanes]
            delta = jnp.sum(stacked(prod[:, lanes]), axis=1, keepdims=True)
            total = dp.shape[0]
            own = dot_nt(stacked(dp[:tok]), vp)
            oth = dot_nt(stacked(dp[tok:]), vp[:tok])
            for half in range(2):
                head = heads * group + 2 * pair + half
                dh = delta[half * total:(half + 1) * total]
                ds = wo_ref[head].astype(F32) * (own[half * tok:(half + 1) * tok] - dh[:tok])
                rows_ref[pl.ds(head, 1), :] = jnp.sum(ds * same, axis=0, keepdims=True)
                rows_ref[pl.ds(HEADS + head, 1), :] = jnp.sum(ds, axis=0, keepdims=True)
                so_ref[head] = ds.astype(BF)
                down = oth[half * rest_rows:(half + 1) * rest_rows]
                sx_ref[head] = (wx_ref[head].astype(F32) * (down - dh[tok:])).astype(BF)

    each_group(tok + rest_rows, body)
    col = jnp.sum(rows_ref[...], axis=1, keepdims=True)
    col = jnp.concatenate([col, jnp.zeros((128 - 2 * HEADS, 1), F32)], axis=0)
    sums_ref[...] = jnp.transpose(jnp.broadcast_to(col, (128, 128)))[:1]


def input_grad_kernel(qvo_ref, qvx_ref, ko_ref, kx_ref, co_ref, dc_ref, wo_ref, wx_ref, so_ref, sx_ref,
                      wfull_ref, mixed_ref, qg_ref, kg_ref, vg_ref, acc_ref):
    tok, rest_rows = qvo_ref.shape[0] // 2, qvx_ref.shape[0] // 2
    heads = heads_at_once(tok + rest_rows)
    nb = heads * HEAD_DIM // (2 * wfull_ref.shape[2])
    acc_ref[...] = jnp.zeros_like(acc_ref)

    def side_by_side(own_ref, oth_ref, head):
        return jnp.concatenate(
            [jnp.concatenate([own_ref[h, :, :tok], oth_ref[h]], axis=0) for h in (head, head + 1)], axis=1)

    def body(group, at):
        w = wfull_ref[pl.ds(group * nb, nb)].reshape(heads * HEAD_DIM, wfull_ref.shape[3])
        acc_ref[...] += dot_nn(co_ref[:, at].astype(BF), w)
        q = jnp.concatenate([qvo_ref[:tok, at], qvx_ref[:rest_rows, at]], axis=0) * jnp.asarray(SCALE, BF)
        k = jnp.concatenate([ko_ref[:, at], kx_ref[:, at]], axis=0)
        d = dc_ref[:, at]
        found = []
        for pair in range(heads // 2):
            lanes = slice(pair * PAIR, (pair + 1) * PAIR)
            head = heads * group + 2 * pair
            so = jnp.concatenate([so_ref[head], so_ref[head + 1]], axis=0)
            found.append((unstacked(dot_nn(so, k[:, lanes])) * SCALE,
                          unstacked(dot_tn(side_by_side(so_ref, sx_ref, head), q[:, lanes])),
                          unstacked(dot_tn(side_by_side(wo_ref, wx_ref, head), d[:, lanes]))))
        for ref, parts in zip((qg_ref, kg_ref, vg_ref), zip(*found)):
            ref[:, at] = jnp.concatenate(parts, axis=1).astype(BF)

    each_group(tok + rest_rows, body)
    mixed_ref[...] = acc_ref[...].astype(BF)


def shape(dims, dtype):
    return jax.ShapeDtypeStruct(dims, dtype)


def cost(flops):
    return pl.CostEstimate(flops=flops, bytes_accessed=4 << 20, transcendentals=0)


def plain(kernel, args, outs, flops=1 << 22, scratch=(), in_specs=None, limit=8 << 20):
    spec = pl.BlockSpec(memory_space=pltpu.VMEM)
    return pl.pallas_call(
        kernel, in_specs=in_specs or [spec] * len(args), out_specs=[spec] * len(outs), out_shape=outs,
        scratch_shapes=scratch, compiler_params=pltpu.CompilerParams(vmem_limit_bytes=limit),
        cost_estimate=cost(flops))(*args)


def on_device(queries, keys, values, d_mixed, series_ids, variate_ids, variate_bias, w_out):
    query, key_rows, value_rows, upstream = queries[0], keys[0], values[0], d_mixed[0]
    tok, width = query.shape
    n_ctx, n_dp = lax.axis_size("ctx"), lax.axis_size("dp")
    total, cols, block = tok * n_ctx, width // n_ctx, width // n_dp
    rest = total - tok
    bits = [1 << i for i in range(n_dp.bit_length() - 1)]
    assert 1 << len(bits) == n_dp and len(bits) > 3 and n_ctx > 1

    def swap(array, bit):
        return lax.ppermute(array, "dp", [(i, i ^ bit) for i in range(n_dp)])

    def turns(array):
        return [lax.ppermute(array, "ctx", [(i, (i + by) % n_ctx) for i in range(n_ctx)])
                for by in range(1, n_ctx)]

    def others(array, axis):
        parts = turns(array)
        return parts[0] if len(parts) == 1 else jnp.concatenate(parts, axis=axis)

    hbm = pl.BlockSpec(memory_space=pltpu.HBM)
    limit = (12 << 20) + 40 * total * width
    kx = others(key_rows, 0)
    local = [variate_bias, series_ids, variate_ids, upstream, query, key_rows, value_rows]
    cut = shape((tok, cols), BF)
    code, gaps, upstream, qv, key_rows, *cuts = plain(
        prepare_kernel, [pltpu.with_memory_space_constraint(a, pltpu.HBM) for a in local],
        [shape(series_ids.shape, jnp.int32), shape((HEADS, 128), F32), shape((tok, width), BF),
         shape((2 * tok, width), BF), shape((tok, width), BF)] + [cut] * n_ctx,
        scratch=[pltpu.VMEM((2, HEADS), F32), pltpu.VMEM((2, 1, tok), jnp.int32), pltpu.SemaphoreType.DMA((len(local),))],
        in_specs=[hbm] * len(local))
    code_x = others(code, 1)
    parts = turns(qv)
    qvx = parts[0] if n_ctx == 2 else jnp.concatenate([p[:tok] for p in parts] + [p[tok:] for p in parts])
    near = [lax.ppermute(part, "ctx", [(i, (i + by) % n_ctx) for i in range(n_ctx)])
            for by, part in enumerate(cuts[:-1], 1)]
    near = near[0] if len(near) == 1 else jnp.concatenate(near, axis=0)
    dx = [near, *turns(cuts[-1])] if n_ctx == 2 else [others(upstream, 0)]

    pieces = {0: w_out}
    for bit in reversed(bits):
        for piece in list(pieces):
            pieces[piece ^ bit] = swap(pieces[piece], bit)
    order = list(pieces)

    o_shape, x_shape = shape((HEADS, tok, total), BF), shape((HEADS, rest, tok), BF)

    ctx_o, ctx_x, w_o, w_x = plain(
        forward_kernel, [gaps, code, code_x, qv, qvx, key_rows, kx],
        [shape((tok, width), F32), shape((rest, width), F32), o_shape, x_shape],
        16 * HEADS * total * total * HEAD_DIM, [pltpu.VMEM((total, total), F32)] * 2, limit=limit)
    blocks, rows = shape((n_dp // 4, block, cols), F32), shape((width // 4, cols), BF)
    go, stay, send_go, send_stay = plain(weight_kernel, [ctx_o, ctx_x, upstream, near], [blocks] * 2 + [rows] * 2,
                                         2 * total * width * cols, limit=limit)
    send, = plain(sum_kernel, [go, swap(send_go, 1)], [rows])
    keep, = plain(sum_kernel, [stay, swap(send_stay, 1)], [blocks])
    w_full, d_ctx, s_o, s_x, sums = plain(
        functools.partial(score_grad_kernel, order, len(dx)),
        [code, code_x, qv, qvx, ctx_o, ctx_x, w_o, w_x, upstream, *dx, *[pieces[p] for p in order]],
        [shape((n_dp // 2, 2, block, width), BF), shape((total, width), BF), o_shape, x_shape,
         shape((1, 128), F32)], 16 * HEADS * total * total * HEAD_DIM,
        [pltpu.VMEM((tok, total), F32), pltpu.VMEM((total, width), BF), pltpu.VMEM((2 * HEADS, total), F32)],
        limit=limit)

    bits = bits[:2] + bits[:1:-1]
    for bit in bits[:-1]:
        got = swap(sums, bit)
        if bit != bits[-2]:
            sums, = plain(add_kernel, [sums, got], [shape((1, 128), F32)])
    for bit, after in zip(bits[1:], bits[2:]):
        n = keep.shape[0] // 2
        args, outs = [keep, swap(send, bit)], [shape((n, block, cols), F32)]
        if n > 1:
            outs.append(shape((n * block, cols), BF))
        else:
            args += [sums, got]
            outs += [shape((block * cols // 128 + TAIL, 128), BF)] * 2 + [shape((1, 128), F32)]
        keep, send, *last = plain(functools.partial(halve_kernel, after, n if after in bits[2:] else 1), args, outs)
    keep_send, sums = last
    args = [keep, sums, swap(send, bits[-1])]
    for by, part in enumerate(turns(keep_send), 1):
        route = [(c * n_dp + d, (c + by) % n_ctx * n_dp + (d ^ bits[-1])) for c in range(n_ctx) for d in range(n_dp)]
        args += [part, lax.ppermute(send, ("ctx", "dp"), route)]
    w_grad, bias_grad = plain(final_kernel, args, [shape((block, width), F32), shape((2, HEADS), F32)])
    mixed, q_grad, k_grad, v_grad = plain(
        input_grad_kernel, [qv, qvx, key_rows, kx, ctx_o, d_ctx, w_o, w_x, s_o, s_x, w_full],
        [shape((tok, width), BF)] * 4, 16 * HEADS * total * total * HEAD_DIM,
        [pltpu.VMEM((tok, width), F32)], limit=limit)
    return mixed[None], q_grad[None], k_grad[None], v_grad[None], w_grad, bias_grad


def solution(mesh):
    data = P("dp", "ctx", None)

    return jax.shard_map(
        on_device,
        mesh=mesh,
        in_specs=(data, data, data, data, P("dp", "ctx"), P("dp", "ctx"), P(), P("dp", None)),
        out_specs=(data, data, data, data, P("dp", None), P()),
        check_vma=False,
    )
```
